8 devices in a mesh: data: 8 (over z, y, x, core).
Axes of the slice: x: 2, y: 2, z: 1, core: 2. Of those that a mesh axis runs over, the one named last changes fastest.
Arguments:
- act_in: bfloat16 [32768, 1536], P('data')
- grad_out: bfloat16 [32768, 1536], P('data')
- w_up1: bfloat16 [1536, 6144], replicated
- w_down1: bfloat16 [6144, 1536], replicated
- w_up2: bfloat16 [1536, 6144], replicated
- w_down2: bfloat16 [6144, 1536], replicated
- master_up1: float32 [1536, 6144], P('data')
- master_down1: float32 [6144, 1536], P('data')
- master_up2: float32 [1536, 6144], P('data')
- master_down2: float32 [6144, 1536], P('data')
- mom_up1: float32 [1536, 6144], P('data')
- mom_down1: float32 [6144, 1536], P('data')
- mom_up2: float32 [1536, 6144], P('data')
- mom_down2: float32 [6144, 1536], P('data')
- vel_up1: float32 [1536, 6144], P('data')
- vel_down1: float32 [6144, 1536], P('data')
- vel_up2: float32 [1536, 6144], P('data')
- vel_down2: float32 [6144, 1536], P('data')
- learn_rate: float32 [], replicated
- clip_norm: float32 [], replicated
Outputs:
- output 1: bfloat16 [1536, 6144], replicated
- output 2: bfloat16 [6144, 1536], replicated
- output 3: bfloat16 [1536, 6144], replicated
- output 4: bfloat16 [6144, 1536], replicated
- output 5: float32 [1536, 6144], P('data')
- output 6: float32 [6144, 1536], P('data')
- output 7: float32 [1536, 6144], P('data')
- output 8: float32 [6144, 1536], P('data')
- output 9: float32 [1536, 6144], P('data')
- output 10: float32 [6144, 1536], P('data')
- output 11: float32 [1536, 6144], P('data')
- output 12: float32 [6144, 1536], P('data')
- output 13: float32 [1536, 6144], P('data')
- output 14: float32 [6144, 1536], P('data')
- output 15: float32 [1536, 6144], P('data')
- output 16: float32 [6144, 1536], P('data')
- output 17: float32 [], replicated
All inputs are finite; a program needn't handle non-finite values.
Results may differ from the reference program's by a relative error of at most 0.0109188.
Values are sent between devices in bfloat16 or wider.
A program may use at most 1.25 GiB of HBM per device.

```python
import math
import jax
import jax.numpy as jnp
from jax import lax

D = 1536
FF = 6144
ROWS = 32768
GROUP = 8
STEP = 20
SAMPLE = 256

BETA_ONE = 0.9
BETA_TWO = 0.95
EPSILON = 1e-8
NORM_EPS = 1e-6
CORR_ONE = 1.0 - BETA_ONE ** STEP
CORR_TWO = 1.0 - BETA_TWO ** STEP
ROOT_HALF = math.sqrt(0.5)
INV_ROOT_TAU = 1.0 / math.sqrt(2.0 * math.pi)
LAYER_GAINS = (1.0, 1.5, 1.0, 2.0)
LAYER_NAMES = ("up1", "down1", "up2", "down2")


def gelu_pair(pre):
    normal_cdf = 0.5 * (1.0 + lax.erf(pre * ROOT_HALF))
    density = jnp.exp(-0.5 * pre * pre) * INV_ROOT_TAU
    return pre * normal_cdf, normal_cdf + pre * density


def fwd_bwd(rows_in, rows_grad, w_up1, w_down1, w_up2, w_down2):
    pre_up1 = jnp.dot(rows_in, w_up1, preferred_element_type=jnp.float32)
    gel_up1, der_up1 = gelu_pair(pre_up1)
    act_up1 = gel_up1.astype(jnp.bfloat16)
    mid_act = jnp.dot(act_up1, w_down1, preferred_element_type=jnp.float32).astype(jnp.bfloat16)
    pre_up2 = jnp.dot(mid_act, w_up2, preferred_element_type=jnp.float32)
    gel_up2, der_up2 = gelu_pair(pre_up2)
    act_up2 = gel_up2.astype(jnp.bfloat16)
    grad_act2 = jnp.dot(rows_grad, w_down2.T, preferred_element_type=jnp.float32).astype(jnp.bfloat16)
    grad_pre2 = (grad_act2.astype(jnp.float32) * der_up2).astype(jnp.bfloat16)
    grad_mid = jnp.dot(grad_pre2, w_up2.T, preferred_element_type=jnp.float32).astype(jnp.bfloat16)
    grad_act1 = jnp.dot(grad_mid, w_down1.T, preferred_element_type=jnp.float32).astype(jnp.bfloat16)
    grad_pre1 = (grad_act1.astype(jnp.float32) * der_up1).astype(jnp.bfloat16)
    return ((act_up2, rows_grad), (mid_act, grad_pre2), (act_up1, grad_mid), (rows_in, grad_pre1))


def adam_step(grad_rows, master_old, mom_old, vel_old, clip_scale, learn_rate):
    scaled = clip_scale * grad_rows
    mom_new = BETA_ONE * mom_old + (1.0 - BETA_ONE) * scaled
    vel_new = BETA_TWO * vel_old + (1.0 - BETA_TWO) * scaled * scaled
    master_new = master_old - learn_rate * (mom_new / CORR_ONE) / (jnp.sqrt(vel_new / CORR_TWO) + EPSILON)
    return master_new.astype(jnp.bfloat16), master_new, mom_new, vel_new


def norm_estimate(act_in, grad_out, weights):
    stride = ROWS // SAMPLE
    grad_pairs = fwd_bwd(act_in[::stride], grad_out[::stride], weights[0], weights[1], weights[2], weights[3])
    row_total = 0.0
    for layer_in, layer_delta in grad_pairs:
        in_sq = jnp.sum(jnp.square(layer_in.astype(jnp.float32)), axis=1)
        delta_sq = jnp.sum(jnp.square(layer_delta.astype(jnp.float32)), axis=1)
        row_total = row_total + jnp.sum(in_sq * delta_sq)
    return jnp.sqrt(row_total * stride) / GROUP


def setup_inputs(seed: int = 0) -> dict:
    key_list = jax.random.split(jax.random.key(seed), 20)
    act_in = jax.random.normal(key_list[0], (ROWS, D), jnp.float32).astype(jnp.bfloat16)
    grad_scale = 2.0 * GROUP / math.sqrt(ROWS * D * FF)
    grad_out = (grad_scale * jax.random.normal(key_list[1], (ROWS, D), jnp.float32)).astype(jnp.bfloat16)
    shapes = ((D, FF), (FF, D), (D, FF), (FF, D))
    weights = []
    masters = []
    for layer_idx in range(4):
        init_scale = LAYER_GAINS[layer_idx] / math.sqrt(shapes[layer_idx][0])
        weight = init_scale * jax.random.normal(key_list[2 + layer_idx], shapes[layer_idx], jnp.float32)
        weights.append(weight.astype(jnp.bfloat16))
        masters.append(weight + 0.01 * init_scale * jax.random.normal(key_list[6 + layer_idx], shapes[layer_idx], jnp.float32))
    clip_norm = norm_estimate(act_in, grad_out, weights) * jax.random.uniform(key_list[10], (), jnp.float32, 0.3, 0.6)
    unit_size = clip_norm / math.sqrt(4 * D * FF)
    inputs = {"act_in": act_in, "grad_out": grad_out}
    for layer_idx in range(4):
        inputs["w_" + LAYER_NAMES[layer_idx]] = weights[layer_idx]
    for layer_idx in range(4):
        inputs["master_" + LAYER_NAMES[layer_idx]] = masters[layer_idx]
    for layer_idx in range(4):
        inputs["mom_" + LAYER_NAMES[layer_idx]] = 0.1 * unit_size * jax.random.normal(key_list[11 + layer_idx], shapes[layer_idx], jnp.float32)
    for layer_idx in range(4):
        inputs["vel_" + LAYER_NAMES[layer_idx]] = 0.05 * unit_size * unit_size * jax.random.uniform(key_list[15 + layer_idx], shapes[layer_idx], jnp.float32, 0.5, 1.5)
    inputs["learn_rate"] = 0.5 / math.sqrt(D) * jax.random.uniform(key_list[19], (), jnp.float32, 0.2, 1.0)
    inputs["clip_norm"] = clip_norm
    return inputs


def reference(act_in, grad_out, w_up1, w_down1, w_up2, w_down2, master_up1, master_down1, master_up2, master_down2, mom_up1, mom_down1, mom_up2, mom_down2, vel_up1, vel_down1, vel_up2, vel_down2, learn_rate, clip_norm):
    rows_dev = ROWS // GROUP
    dev_in = act_in.reshape(GROUP, rows_dev, D)
    dev_grad = grad_out.reshape(GROUP, rows_dev, D)

    def accumulate(carry, block):
        grad_pairs = fwd_bwd(block[0], block[1], w_up1, w_down1, w_up2, w_down2)
        summed = tuple(carry[layer_idx] + jnp.dot(grad_pairs[layer_idx][0].T, grad_pairs[layer_idx][1], preferred_element_type=jnp.float32) for layer_idx in range(4))
        return summed, None

    start_sums = (jnp.zeros((FF, D), jnp.float32), jnp.zeros((D, FF), jnp.float32), jnp.zeros((FF, D), jnp.float32), jnp.zeros((D, FF), jnp.float32))
    totals = lax.scan(accumulate, start_sums, (dev_in, dev_grad))[0]
    grad_list = [totals[3] / GROUP, totals[2] / GROUP, totals[1] / GROUP, totals[0] / GROUP]
    grad_norm = jnp.sqrt(sum(jnp.sum(grad_rows * grad_rows) for grad_rows in grad_list))
    clip_scale = jnp.minimum(1.0, clip_norm / (grad_norm + NORM_EPS))
    state_up1 = adam_step(grad_list[0], master_up1, mom_up1, vel_up1, clip_scale, learn_rate)
    state_down1 = adam_step(grad_list[1], master_down1, mom_down1, vel_down1, clip_scale, learn_rate)
    state_up2 = adam_step(grad_list[2], master_up2, mom_up2, vel_up2, clip_scale, learn_rate)
    state_down2 = adam_step(grad_list[3], master_down2, mom_down2, vel_down2, clip_scale, learn_rate)
    return (state_up1[0], state_down1[0], state_up2[0], state_down2[0], state_up1[1], state_down1[1], state_up2[1], state_down2[1], state_up1[2], state_down1[2], state_up2[2], state_down2[2], state_up1[3], state_down1[3], state_up2[3], state_down2[3], grad_norm)
```

```python
import functools
import math

import jax
import jax.numpy as jnp
from jax import lax
from jax.experimental import pallas as pl
from jax.experimental.pallas import tpu as pltpu
from jax.sharding import PartitionSpec as P

STEP = 20
BETA_ONE = 0.9
BETA_TWO = 0.95
EPSILON = 1e-8
NORM_EPS = 1e-6
CORR_ONE = 1.0 - BETA_ONE ** STEP
CORR_TWO = 1.0 - BETA_TWO ** STEP
ROOT_HALF = math.sqrt(0.5)
EXP_SCALE = -0.5 * math.log2(math.e)
EXP_SHIFT = -0.5 * math.log2(2.0 * math.pi)

F32 = jnp.float32
BF16 = jnp.bfloat16
MESH = pl.DeviceIdType.MESH
ANY = pl.BlockSpec(memory_space=pl.ANY)
VMEM_LIMIT = 67043328
D = 1536
FF = 6144
TILE = 256
X_PAIRS = [(i, i ^ 2) for i in range(8)]
Y_PAIRS = [(i, i ^ 4) for i in range(8)]
C_PAIRS = [(i, i ^ 1) for i in range(8)]


def dot_nn(a, b):
    return lax.dot_general(a, b, (((1,), (0,)), ((), ())), preferred_element_type=F32)


def dot_nt(a, b):
    return lax.dot_general(a, b, (((1,), (1,)), ((), ())), preferred_element_type=F32)


def dot_tn(a, b):
    return lax.dot_general(a, b, (((0,), (0,)), ((), ())), preferred_element_type=F32)


def normal_cdf(z):
    return 0.5 * lax.erf(z * ROOT_HALF) + 0.5


def gelu_slope(z, cdf):
    return cdf + z * jnp.exp2(z * z * EXP_SCALE + EXP_SHIFT)


def params(**kw):
    return pltpu.CompilerParams(vmem_limit_bytes=VMEM_LIMIT, **kw)


def cost(units, mib):
    return pl.CostEstimate(flops=int(units * 2 * 4096 * D * FF), bytes_accessed=mib * 2 ** 20, transcendentals=0)


def place():
    me = lax.axis_index("data")
    core = me % 2
    chip = me // 2
    return me, core, chip % 2, chip // 2


def front_kernel(x_ref, w1_hbm, w2_hbm, h_ref, z_ref, u_ref, w1_v, w2_v, sem):
    step = pl.program_id(0)
    n1, n2 = 1024, 512

    def loads():
        one = [pltpu.make_async_copy(w1_hbm.at[:, n:n + n1], w1_v.at[:, n:n + n1], sem.at[i])
               for i, n in enumerate(range(0, FF, n1))]
        two = [pltpu.make_async_copy(w2_hbm.at[:, n:n + n2], w2_v.at[:, n:n + n2], sem.at[FF // n1 + i])
               for i, n in enumerate(range(0, D, n2))]
        return one, two

    def work(first):
        one, two = loads()
        if first:
            for c in one + two:
                c.start()
        for n in range(0, FF, 512):
            if first and n % n1 == 0:
                one[n // n1].wait()
            z = dot_nn(x_ref[...], w1_v[:, n:n + 512])
            h_ref[:, n:n + 512] = (z * normal_cdf(z)).astype(BF16)
            z_ref[:, n:n + 512] = z
        for n in range(0, D, n2):
            if first:
                two[n // n2].wait()
            u_ref[:, n:n + n2] = dot_nn(h_ref[...], w2_v[:, n:n + n2]).astype(BF16)

    @pl.when(step == 0)
    def _():
        work(True)

    @pl.when(step > 0)
    def _():
        work(False)


def front(x, w1, w2):
    rows = x.shape[0]
    bm = 256
    return pl.pallas_call(
        front_kernel,
        grid=(rows // bm,),
        in_specs=[pl.BlockSpec((bm, D), lambda i: (i, 0)), ANY, ANY],
        out_specs=[pl.BlockSpec((bm, FF), lambda i: (i, 0)), pl.BlockSpec((bm, FF), lambda i: (i, 0)),
                   pl.BlockSpec((bm, D), lambda i: (i, 0))],
        out_shape=[jax.ShapeDtypeStruct((rows, FF), BF16), jax.ShapeDtypeStruct((rows, FF), F32),
                   jax.ShapeDtypeStruct((rows, D), BF16)],
        scratch_shapes=[pltpu.VMEM((D, FF), BF16), pltpu.VMEM((FF, D), BF16), pltpu.SemaphoreType.DMA((9,))],
        compiler_params=params(), cost_estimate=cost(2, 220), name="front",
    )(x, w1, w2)


TILES = 24
LAG = 2


def fused_kernel(mid, a_hbm, b_hbm, w_ref, *rest):
    if mid:
        w4_ref, q_at, *rest = rest
    else:
        z_ref, h_at, *rest = rest
    (stay4, near4, fin4, stay3, near3, fin3, a_v, b_v, hidden_v, raw4, raw3, got4, got3, far4, far3,
     load_sem, send4, send3, recv4, recv3, done4, done3, recv_far4, recv_far3, recv_hbm) = rest
    if mid:
        h_at = hidden_v
    else:
        q_at = hidden_v
    step = pl.program_id(0)
    me, core, px, py = place()
    partner = me + 1 - 2 * core
    x_dev = me + 2 - 4 * px
    y_dev = me + 4 - 8 * py
    own_chip = py * 2 + px
    x_chip = py * 2 + 1 - px
    y_chip = (1 - py) * 2 + px
    part = 1024
    ring = got3.shape[0]
    slack = ring - 4

    def remote(src, dst, send, recv, dev):
        return pltpu.make_async_remote_copy(src_ref=src, dst_ref=dst, send_sem=send, recv_sem=recv,
                                            device_id=(dev,), device_id_type=MESH)

    def drain(ref, sem):
        pltpu.make_async_copy(ref, ref, sem).wait()

    def loads():
        return [[pltpu.make_async_copy(hbm.at[i:i + part], v.at[i:i + part], load_sem.at[k, i // part])
                 for i in range(0, 4096, part)] for k, (hbm, v) in enumerate(((a_hbm, a_v), (b_hbm, b_v)))]

    def mine(s):
        return (s // 4) % 2 == core

    def role(s):
        return (s + px) % 2 + 2 * ((s // 2 + py) % 2)

    def share3(s):
        return remote(raw3.at[s % 2, :, 1 - core], got3.at[s % ring], send3.at[s % 2], recv3.at[s % ring], partner)

    def share4(s):
        return remote(raw4.at[s % 2], got4.at[s % 4], send4.at[s % 2], recv4.at[s % 4], partner)

    def legs3(s):
        odd = s % 2
        first = x_dev + odd * (y_dev - x_dev)
        second = y_dev + odd * (x_dev - y_dev)
        near = x_chip + odd * (y_chip - x_chip)
        far = y_chip + odd * (x_chip - y_chip)
        blk = got3.at[s % ring]
        sem = done3.at[s % ring]
        return (remote(blk.at[x_chip + y_chip - own_chip], far3.at[s % 4], sem, recv_far3.at[s % 4], first),
                remote(blk.at[near], near3.at[s], sem, recv_hbm.at[0], first),
                pltpu.make_async_copy(blk.at[own_chip], stay3.at[s], sem),
                remote(blk.at[far], fin3.at[s], sem, recv_hbm.at[1], second), far)

    def halves(s):
        return [(got4.at[s % 4, :, k * 768:k * 768 + 768], done4.at[s % 4]) for k in range(2)]

    def first4(s):
        t = s // 8
        r = role(s)
        for k, (blk, sem) in enumerate(halves(s)):
            dev = y_dev if k else x_dev

            @pl.when(r == 3)
            def _():
                remote(blk, far4.at[k], sem, recv_far4.at[k], dev).start()

            @pl.when(r == 1 + k)
            def _():
                remote(blk, near4.at[k, t], sem, recv_hbm.at[2], dev).start()

            @pl.when(r == 0)
            def _():
                pltpu.make_async_copy(blk, stay4.at[k, t], sem).start()

    def second4(s):
        t = s // 8
        r = role(s)
        for k, (blk, sem) in enumerate(halves(s)):
            @pl.when(r == 2 - k)
            def _():
                drain(far4.at[k], recv_far4.at[k])
                blk[...] = blk[...] + far4[k]
                remote(blk, fin4.at[k, t], sem, recv_hbm.at[3], x_dev if k else y_dev).start()

    def add3(s):
        for q in range(4):
            got3[s % ring, q] = got3[s % ring, q] + raw3[s % 2, q, core]

    def fold3(s):
        far = legs3(s)[4]
        got3[s % ring, far] = got3[s % ring, far] + far3[s % 4]

    def hidden(first):
        cps = loads() if first else None
        if first:
            for pair in zip(*cps):
                for c in pair:
                    c.start()
        for i in range(0, 4096, 256):
            if first and i % part == 0:
                cps[1][i // part].wait()
                if mid:
                    cps[0][i // part].wait()
            rows = slice(i, i + 256)
            if mid:
                z = dot_nn(a_v[rows], w_ref[...])
                e = dot_nt(b_v[rows], w4_ref[...]).astype(BF16)
                cdf = normal_cdf(z)
                h_at[rows] = (z * cdf).astype(BF16)
            else:
                e = dot_nt(b_v[rows], w_ref[...]).astype(BF16)
                z = z_ref[rows]
                cdf = normal_cdf(z)
            q_at[rows] = (e.astype(F32) * gelu_slope(z, cdf)).astype(BF16)
        if first and not mid:
            for c in cps[0]:
                c.wait()

    def dot4():
        raw4[step % 2] = dot_tn(h_at[...], b_v[...])

    both = jnp.logical_and
    prev = step - 1
    old = prev - LAG
    gone = old - slack
    live = step < TILES
    fresh = both(step >= 1, step <= TILES)

    @pl.when(step == 0)
    def _():
        bar = pltpu.get_barrier_semaphore()
        for dev in (partner, x_dev, y_dev):
            pl.semaphore_signal(bar, inc=1, device_id=(dev,), device_id_type=MESH)
        pl.semaphore_wait(bar, 3)
        hidden(True)

    @pl.when(both(step > 0, live))
    def _():
        hidden(False)

    @pl.when(both(step >= 2, step < TILES + 2))
    def _():
        share3(step - 2).wait_send()

        @pl.when(jnp.logical_not(mine(step - 2)))
        def _():
            share4(step - 2).wait_send()

    def settle(s):
        drain(got3.at[s % ring], done3.at[s % ring])

        @pl.when(mine(s))
        def _():
            drain(got4.at[s % 4], done4.at[s % 4])

    @pl.when(gone >= 0)
    def _():
        settle(gone)

    @pl.when(fresh)
    def _():
        share3(prev).wait_recv()

        @pl.when(mine(prev))
        def _():
            share4(prev).wait_recv()
            got4[prev % 4] = got4[prev % 4] + raw4[prev % 2]

    @pl.when(old >= 0)
    def _():
        drain(far3.at[old % 4], recv_far3.at[old % 4])

    @pl.when(both(old >= 0, live))
    def _():
        add3(prev)
        fold3(old)
        dot4()

    @pl.when(old < 0)
    def _():
        dot4()

    @pl.when(both(fresh, jnp.logical_or(old < 0, step == TILES)))
    def _():
        add3(prev)

    @pl.when(step >= TILES)
    def _():
        fold3(old)

    @pl.when(old >= 0)
    def _():
        legs3(old)[3].start()

        @pl.when(mine(old))
        def _():
            second4(old)

    @pl.when(fresh)
    def _():
        for c in legs3(prev)[:3]:
            c.start()

        @pl.when(mine(prev))
        def _():
            first4(prev)

    @pl.when(both(live, jnp.logical_not(mine(step))))
    def _():
        share4(step).start()

    @pl.when(live)
    def _():
        g3 = dot_tn(a_v[...], q_at[...])
        for q in range(4):
            for c in range(2):
                at = q * 384 + c * 192
                raw3[step % 2, q, c] = g3[at:at + 192]
        share3(step).start()

    @pl.when(step == TILES + LAG)
    def _():
        for s in range(TILES - slack, TILES):
            settle(s)
        for k, ref in enumerate((near3, fin3, near4, fin4)):
            drain(ref, recv_hbm.at[k])


def fused(mid, a, b, *more):
    rows = a.shape[0]
    ring = 6 if mid else 5

    def tile(s):
        s = jnp.minimum(s, TILES - 1)
        return (2 * (s % 4) + s // 4 % 2) * 3 + s // 8

    down_w = pl.BlockSpec((TILE, D), lambda s: (tile(s), 0))
    up_w = pl.BlockSpec((D, TILE), lambda s: (0, tile(s)))
    wide = pl.BlockSpec((rows, TILE), lambda s: (0, tile(s)))
    g4 = jax.ShapeDtypeStruct((2, 3, 256, 768), F32)
    g3 = jax.ShapeDtypeStruct((TILES, 192, TILE), F32)
    dma = pltpu.SemaphoreType.DMA
    return pl.pallas_call(
        functools.partial(fused_kernel, mid),
        grid=(TILES + 1 + LAG,),
        in_specs=[ANY, ANY] + ([up_w, down_w] if mid else [down_w, wide, wide]),
        out_specs=([wide] if mid else []) + [ANY] * 6,
        out_shape=([jax.ShapeDtypeStruct((rows, FF), BF16)] if mid else []) + [g4] * 3 + [g3] * 3,
        scratch_shapes=[pltpu.VMEM((rows, D), BF16), pltpu.VMEM((rows, D), BF16), pltpu.VMEM((rows, TILE), BF16),
                        pltpu.VMEM((2, TILE, D), F32), pltpu.VMEM((2, 4, 2, 192, TILE), F32),
                        pltpu.VMEM((4, TILE, D), F32), pltpu.VMEM((ring, 4, 192, TILE), F32),
                        pltpu.VMEM((2, TILE, 768), F32), pltpu.VMEM((4, 192, TILE), F32),
                        dma((2, 4)), dma((2,)), dma((2,)), dma((4,)), dma((ring,)), dma((4,)), dma((ring,)),
                        dma((2,)), dma((4,)), dma((4,))],
        compiler_params=params(collective_id=int(mid), has_side_effects=True),
        cost_estimate=cost(4 if mid else 3, 300), name="middle" if mid else "last",
    )(a, b, *more)


def back_kernel(q_ref, w_ref, o_ref):
    o_ref[...] = dot_nt(q_ref[...], w_ref[...]).astype(BF16)


def back(q, w3):
    rows = q.shape[0]
    bm, bn = 512, 768
    return pl.pallas_call(
        back_kernel,
        grid=(D // bn, rows // bm),
        in_specs=[pl.BlockSpec((bm, FF), lambda j, i: (i, 0)), pl.BlockSpec((bn, FF), lambda j, i: (j, 0))],
        out_specs=pl.BlockSpec((bm, bn), lambda j, i: (i, j)),
        out_shape=jax.ShapeDtypeStruct((rows, D), BF16),
        compiler_params=params(), cost_estimate=cost(1, 130), name="back",
    )(q, w3)


def total_kernel(v_ref, o_ref, all_v, send, recv):
    me = lax.axis_index("data")
    bar = pltpu.get_barrier_semaphore()
    for k in range(1, 8):
        pl.semaphore_signal(bar, inc=1, device_id=((me + k) % 8,), device_id_type=MESH)
    pl.semaphore_wait(bar, 7)
    copies = []
    for k in range(1, 8):
        copies.append(pltpu.make_async_remote_copy(
            src_ref=v_ref, dst_ref=all_v.at[me], send_sem=send.at[k], recv_sem=recv.at[me],
            device_id=((me + k) % 8,), device_id_type=MESH))
    for c in copies:
        c.start()
    all_v[me] = v_ref[...]
    for k in range(1, 8):
        src = (me + k) % 8
        pltpu.make_async_copy(all_v.at[src], all_v.at[src], recv.at[src]).wait()
    o_ref[...] = ((all_v[0] + all_v[1]) + (all_v[2] + all_v[3])) + ((all_v[4] + all_v[5]) + (all_v[6] + all_v[7]))
    for c in copies:
        c.wait_send()


def total(value, ident):
    spec = pl.BlockSpec(memory_space=pltpu.VMEM)
    out = pl.pallas_call(
        total_kernel,
        in_specs=[spec], out_specs=spec,
        out_shape=jax.ShapeDtypeStruct((8, 128), F32),
        scratch_shapes=[pltpu.VMEM((8, 8, 128), F32), pltpu.SemaphoreType.DMA((8,)), pltpu.SemaphoreType.DMA((8,))],
        compiler_params=pltpu.CompilerParams(collective_id=ident, has_side_effects=True), name="total",
    )(jnp.broadcast_to(value, (8, 128)))
    return out[0, 0]


def by_x(v):
    return lax.ppermute(v, "data", X_PAIRS)


def by_y(v):
    return lax.ppermute(v, "data", Y_PAIRS)


def by_core(v):
    return lax.ppermute(v, "data", C_PAIRS)


def gather(own):
    rows, cols = own.shape
    me = lax.axis_index("data")
    half = rows // 2
    at_x, at_y = by_x(own), by_y(own)
    diag_a = by_y(at_x[:half])
    diag_b = by_x(at_y[half:])
    blocks = [(0, 0, own), (2, 0, at_x), (4, 0, at_y), (6, 0, diag_a), (6, half, diag_b)]
    out = jnp.zeros((rows * 8, cols), own.dtype)
    for r, off, blk in blocks:
        out = lax.dynamic_update_slice(out, blk, ((me ^ r) * rows + off, 0))
        out = lax.dynamic_update_slice(out, by_core(blk), ((me ^ r ^ 1) * rows + off, 0))
    return out


def adam_step(grad_rows, master_old, mom_old, vel_old, scale, learn_rate):
    scaled = scale * grad_rows
    mom_new = BETA_ONE * mom_old + (1.0 - BETA_ONE) * scaled
    vel_new = BETA_TWO * vel_old + (1.0 - BETA_TWO) * scaled * scaled
    master_new = master_old - learn_rate * (mom_new / CORR_ONE) / (jnp.sqrt(vel_new / CORR_TWO) + EPSILON)
    return master_new.astype(BF16), master_new, mom_new, vel_new


def solution(mesh):
    groups = mesh.shape["data"]
    rows_spec = P("data", None)
    full_spec = P(None, None)
    scalar_spec = P()

    def shard_body(act_in, grad_out, w_up1, w_down1, w_up2, w_down2, master_up1, master_down1, master_up2, master_down2,
                   mom_up1, mom_down1, mom_up2, mom_down2, vel_up1, vel_down1, vel_up2, vel_down2, learn_rate, clip_norm):
        h1, z1, u = front(act_in, w_up1, w_down1)
        q2, *parts = fused(True, u, grad_out, w_up2, w_down2)
        sums = [parts[k] + parts[k + 1] + parts[k + 2] for k in (0, 3)]
        eu = back(q2, w_up2)
        parts = fused(False, act_in, eu, w_down1, z1, h1)
        sums += [parts[k] + parts[k + 1] + parts[k + 2] for k in (0, 3)]
        sumsq = sum(jnp.sum(v * v) for v in sums)
        grad_norm = jnp.sqrt(total(sumsq, 2)) / groups
        scale = jnp.minimum(1.0, clip_norm / (grad_norm + NORM_EPS)) / groups
        g_down2, g_down1 = [v.transpose(1, 2, 0, 3).reshape(768, D) for v in sums[::2]]
        g_up2, g_up1 = [v.reshape(3, 2, 4, 192, TILE).transpose(3, 2, 1, 0, 4).reshape(192, FF) for v in sums[1::2]]
        grads = (g_up1, g_down1, g_up2, g_down2)
        masters = (master_up1, master_down1, master_up2, master_down2)
        moms = (mom_up1, mom_down1, mom_up2, mom_down2)
        vels = (vel_up1, vel_down1, vel_up2, vel_down2)
        states = [adam_step(grads[i], masters[i], moms[i], vels[i], scale, learn_rate) for i in range(4)]
        weights = [gather(s[0]) for s in states]
        results = weights
        for f in range(1, 4):
            results = results + [s[f] for s in states]
        return tuple(results + [grad_norm])

    in_specs = (rows_spec, rows_spec) + (full_spec,) * 4 + (rows_spec,) * 12 + (scalar_spec, scalar_spec)
    out_specs = (full_spec,) * 4 + (rows_spec,) * 12 + (scalar_spec,)
    return jax.shard_map(shard_body, mesh=mesh, in_specs=in_specs, out_specs=out_specs, check_vma=False)
```

```python
import functools
import math

import jax
import jax.numpy as jnp
from jax import lax
from jax.experimental import pallas as pl
from jax.experimental.pallas import tpu as pltpu
from jax.sharding import PartitionSpec as P

STEP = 20
BETA_ONE = 0.9
BETA_TWO = 0.95
EPSILON = 1e-8
NORM_EPS = 1e-6
CORR_ONE = 1.0 - BETA_ONE ** STEP
CORR_TWO = 1.0 - BETA_TWO ** STEP
ROOT_HALF = math.sqrt(0.5)
EXP_SCALE = -0.5 * math.log2(math.e)
EXP_SHIFT = -0.5 * math.log2(2.0 * math.pi)

F32 = jnp.float32
BF16 = jnp.bfloat16
MESH = pl.DeviceIdType.MESH
ANY = pl.BlockSpec(memory_space=pl.ANY)
VMEM_LIMIT = 67043328
D = 1536
FF = 6144
TILE = 256
X_PAIRS = [(i, i ^ 2) for i in range(8)]
Y_PAIRS = [(i, i ^ 4) for i in range(8)]
C_PAIRS = [(i, i ^ 1) for i in range(8)]


def dot_nn(a, b):
    return lax.dot_general(a, b, (((1,), (0,)), ((), ())), preferred_element_type=F32)


def dot_nt(a, b):
    return lax.dot_general(a, b, (((1,), (1,)), ((), ())), preferred_element_type=F32)


def dot_tn(a, b):
    return lax.dot_general(a, b, (((0,), (0,)), ((), ())), preferred_element_type=F32)


def normal_cdf(z):
    return 0.5 * lax.erf(z * ROOT_HALF) + 0.5


def gelu_slope(z, cdf):
    return cdf + z * jnp.exp2(z * z * EXP_SCALE + EXP_SHIFT)


def params(**kw):
    return pltpu.CompilerParams(vmem_limit_bytes=VMEM_LIMIT, **kw)


def cost(units, mib):
    return pl.CostEstimate(flops=int(units * 2 * 4096 * D * FF), bytes_accessed=mib * 2 ** 20, transcendentals=0)


def place():
    me = lax.axis_index("data")
    core = me % 2
    chip = me // 2
    return me, core, chip % 2, chip // 2


def front_kernel(x_ref, w1_hbm, w2_hbm, h_ref, z_ref, u_ref, w1_v, w2_v, sem):
    step = pl.program_id(0)
    n1, n2 = 1024, 512

    def loads():
        one = [pltpu.make_async_copy(w1_hbm.at[:, n:n + n1], w1_v.at[:, n:n + n1], sem.at[i])
               for i, n in enumerate(range(0, FF, n1))]
        two = [pltpu.make_async_copy(w2_hbm.at[:, n:n + n2], w2_v.at[:, n:n + n2], sem.at[FF // n1 + i])
               for i, n in enumerate(range(0, D, n2))]
        return one, two

    def work(first):
        one, two = loads()
        if first:
            for c in one + two:
                c.start()
        for n in range(0, FF, 512):
            if first and n % n1 == 0:
                one[n // n1].wait()
            z = dot_nn(x_ref[...], w1_v[:, n:n + 512])
            h_ref[:, n:n + 512] = (z * normal_cdf(z)).astype(BF16)
            z_ref[:, n:n + 512] = z
        for n in range(0, D, n2):
            if first:
                two[n // n2].wait()
            u_ref[:, n:n + n2] = dot_nn(h_ref[...], w2_v[:, n:n + n2]).astype(BF16)

    @pl.when(step == 0)
    def _():
        work(True)

    @pl.when(step > 0)
    def _():
        work(False)


def front(x, w1, w2):
    rows = x.shape[0]
    bm = 256
    return pl.pallas_call(
        front_kernel,
        grid=(rows // bm,),
        in_specs=[pl.BlockSpec((bm, D), lambda i: (i, 0)), ANY, ANY],
        out_specs=[pl.BlockSpec((bm, FF), lambda i: (i, 0)), pl.BlockSpec((bm, FF), lambda i: (i, 0)),
                   pl.BlockSpec((bm, D), lambda i: (i, 0))],
        out_shape=[jax.ShapeDtypeStruct((rows, FF), BF16), jax.ShapeDtypeStruct((rows, FF), F32),
                   jax.ShapeDtypeStruct((rows, D), BF16)],
        scratch_shapes=[pltpu.VMEM((D, FF), BF16), pltpu.VMEM((FF, D), BF16), pltpu.SemaphoreType.DMA((9,))],
        compiler_params=params(), cost_estimate=cost(2, 220), name="front",
    )(x, w1, w2)


TILES = 24
RING = 8


def fused_kernel(mid, a_hbm, b_hbm, w_ref, *rest):
    if mid:
        w4_ref, q_at, *rest = rest
    else:
        z_hbm, h_hbm, *rest = rest
        *rest, z_ref, h_at, tile_sem = rest
    (stay4, near4, fin4, stay3, near3, fin3, a_v, b_v, hidden_v, raw4, raw3, got4, got3, far4, far3,
     load_sem, send4, send3, recv4, recv3, done4, done3, recv_far4, recv_far3, recv_hbm) = rest
    if mid:
        h_at = hidden_v
    else:
        q_at = hidden_v
    step = pl.program_id(0)
    me, core, px, py = place()
    partner = me + 1 - 2 * core
    x_dev = me + 2 - 4 * px
    y_dev = me + 4 - 8 * py
    own_chip = py * 2 + px
    x_chip = py * 2 + 1 - px
    y_chip = (1 - py) * 2 + px
    part = 1024
    lag = 2 if mid else 4
    slack = RING - lag - 2

    def remote(src, dst, send, recv, dev):
        return pltpu.make_async_remote_copy(src_ref=src, dst_ref=dst, send_sem=send, recv_sem=recv,
                                            device_id=(dev,), device_id_type=MESH)

    def drain(ref, sem):
        pltpu.make_async_copy(ref, ref, sem).wait()

    def loads():
        return [[pltpu.make_async_copy(hbm.at[i:i + part], v.at[i:i + part], load_sem.at[k, i // part])
                 for i in range(0, 4096, part)] for k, (hbm, v) in enumerate(((a_hbm, a_v), (b_hbm, b_v)))]

    def columns(k, s):
        hbm, v = ((z_hbm, z_ref), (h_hbm, h_at))[k]
        return pltpu.make_async_copy(hbm.at[:, pl.ds(pl.multiple_of(tile_of(s) * TILE, TILE), TILE)], v, tile_sem.at[k])

    def following(k):
        if not mid:
            @pl.when(step + 1 < TILES)
            def _():
                columns(k, step + 1).start()

    def mine(s):
        return (s // 4) % 2 == core

    def role(s):
        return (s + px) % 2 + 2 * ((s // 2 + py) % 2)

    def share3(s):
        return remote(raw3.at[s % 2, :, 1 - core], got3.at[s % RING], send3.at[s % 2], recv3.at[s % RING], partner)

    def share4(s):
        return remote(raw4.at[s % 2], got4.at[s % 4], send4.at[s % 2], recv4.at[s % 4], partner)

    def legs3(s):
        odd = s % 2
        first = x_dev + odd * (y_dev - x_dev)
        second = y_dev + odd * (x_dev - y_dev)
        near = x_chip + odd * (y_chip - x_chip)
        far = y_chip + odd * (x_chip - y_chip)
        blk = got3.at[s % RING]
        sem = done3.at[s % RING]
        return (remote(blk.at[x_chip + y_chip - own_chip], far3.at[s % RING], sem, recv_far3.at[s % RING], first),
                remote(blk.at[near], near3.at[s], sem, recv_hbm.at[0], first),
                pltpu.make_async_copy(blk.at[own_chip], stay3.at[s], sem),
                remote(blk.at[far], fin3.at[s], sem, recv_hbm.at[1], second), far)

    def halves(s):
        return [(got4.at[s % 4, :, k * 768:k * 768 + 768], done4.at[s % 4]) for k in range(2)]

    def first4(s):
        t = s // 8
        r = role(s)
        for k, (blk, sem) in enumerate(halves(s)):
            dev = y_dev if k else x_dev

            @pl.when(r == 3)
            def _():
                remote(blk, far4.at[t % 2, k], sem, recv_far4.at[t % 2, k], dev).start()

            @pl.when(r == 1 + k)
            def _():
                remote(blk, near4.at[k, t], sem, recv_hbm.at[2], dev).start()

            @pl.when(r == 0)
            def _():
                pltpu.make_async_copy(blk, stay4.at[k, t], sem).start()

    def second4(s):
        t = s // 8
        r = role(s)
        for k, (blk, sem) in enumerate(halves(s)):
            @pl.when(r == 2 - k)
            def _():
                drain(far4.at[t % 2, k], recv_far4.at[t % 2, k])
                blk[...] = blk[...] + far4[t % 2, k]
                remote(blk, fin4.at[k, t], sem, recv_hbm.at[3], x_dev if k else y_dev).start()

    def add3(s):
        for q in range(4):
            got3[s % RING, q] = got3[s % RING, q] + raw3[s % 2, q, core]

    def fold3(s):
        far = legs3(s)[4]
        got3[s % RING, far] = got3[s % RING, far] + far3[s % RING]

    def hidden(first):
        cps = loads() if first else None
        if first and not mid:
            for k in range(2):
                columns(k, step).start()
        if first:
            for pair in zip(*cps):
                for c in pair:
                    c.start()
        if not mid:
            columns(0, step).wait()
        for i in range(0, 4096, 256):
            if first and i % part == 0:
                cps[1][i // part].wait()
                if mid:
                    cps[0][i // part].wait()
            rows = slice(i, i + 256)
            if mid:
                z = dot_nn(a_v[rows], w_ref[...])
                e = dot_nt(b_v[rows], w4_ref[...]).astype(BF16)
                cdf = normal_cdf(z)
                h_at[rows] = (z * cdf).astype(BF16)
            else:
                e = dot_nt(b_v[rows], w_ref[...]).astype(BF16)
                z = z_ref[rows]
                cdf = normal_cdf(z)
            q_at[rows] = (e.astype(F32) * gelu_slope(z, cdf)).astype(BF16)
        if first and not mid:
            for c in cps[0]:
                c.wait()
        following(0)

    def dot4():
        raw4[step % 2] = dot_tn(h_at[...], b_v[...])

    both = jnp.logical_and
    prev = step - 1
    old = prev - lag
    gone = old - slack
    live = step < TILES
    fresh = both(step >= 1, step <= TILES)

    @pl.when(step == 0)
    def _():
        bar = pltpu.get_barrier_semaphore()
        for dev in (partner, x_dev, y_dev):
            pl.semaphore_signal(bar, inc=1, device_id=(dev,), device_id_type=MESH)
        pl.semaphore_wait(bar, 3)
        hidden(True)

    @pl.when(both(step > 0, live))
    def _():
        hidden(False)

    @pl.when(both(step >= 2, step < TILES + 2))
    def _():
        share3(step - 2).wait_send()

        @pl.when(jnp.logical_not(mine(step - 2)))
        def _():
            share4(step - 2).wait_send()

    def settle(s):
        drain(got3.at[s % RING], done3.at[s % RING])

        @pl.when(mine(s))
        def _():
            drain(got4.at[s % 4], done4.at[s % 4])

    @pl.when(gone >= 0)
    def _():
        settle(gone)

    @pl.when(fresh)
    def _():
        share3(prev).wait_recv()

        @pl.when(mine(prev))
        def _():
            share4(prev).wait_recv()
            got4[prev % 4] = got4[prev % 4] + raw4[prev % 2]

    @pl.when(old >= 0)
    def _():
        drain(far3.at[old % RING], recv_far3.at[old % RING])

    if not mid:
        @pl.when(live)
        def _():
            columns(1, step).wait()

    @pl.when(both(old >= 0, live))
    def _():
        add3(prev)
        fold3(old)
        dot4()
        following(1)

    @pl.when(old < 0)
    def _():
        dot4()
        following(1)

    @pl.when(both(fresh, jnp.logical_or(old < 0, step == TILES)))
    def _():
        add3(prev)

    @pl.when(step >= TILES)
    def _():
        fold3(old)

    @pl.when(old >= 0)
    def _():
        legs3(old)[3].start()

        @pl.when(mine(old))
        def _():
            second4(old)

    @pl.when(fresh)
    def _():
        for c in legs3(prev)[:3]:
            c.start()

        @pl.when(mine(prev))
        def _():
            first4(prev)

    @pl.when(both(live, jnp.logical_not(mine(step))))
    def _():
        share4(step).start()

    @pl.when(live)
    def _():
        g3 = dot_tn(a_v[...], q_at[...])
        for q in range(4):
            for c in range(2):
                at = q * 384 + c * 192
                raw3[step % 2, q, c] = g3[at:at + 192]
        share3(step).start()

    @pl.when(step == TILES + lag)
    def _():
        for s in range(TILES - slack, TILES):
            settle(s)
        for k, ref in enumerate((near3, fin3, near4, fin4)):
            drain(ref, recv_hbm.at[k])


def tile_of(s):
    return (2 * (s % 4) + s // 4 % 2) * 3 + s // 8


def tile(s):
    return tile_of(jnp.minimum(s, TILES - 1))


def fused(mid, a, b, *more):
    rows = a.shape[0]

    down_w = pl.BlockSpec((TILE, D), lambda s: (tile(s), 0))
    up_w = pl.BlockSpec((D, TILE), lambda s: (0, tile(s)))
    wide = pl.BlockSpec((rows, TILE), lambda s: (0, tile(s)))
    g4 = jax.ShapeDtypeStruct((2, 3, 256, 768), F32)
    g3 = jax.ShapeDtypeStruct((TILES, 192, TILE), F32)
    dma = pltpu.SemaphoreType.DMA
    return pl.pallas_call(
        functools.partial(fused_kernel, mid),
        grid=(TILES + (3 if mid else 5),),
        in_specs=[ANY, ANY] + ([up_w, down_w] if mid else [down_w, ANY, ANY]),
        out_specs=([wide] if mid else []) + [ANY] * 6,
        out_shape=([jax.ShapeDtypeStruct((rows, FF), BF16)] if mid else []) + [g4] * 3 + [g3] * 3,
        scratch_shapes=[pltpu.VMEM((rows, D), BF16), pltpu.VMEM((rows, D), BF16), pltpu.VMEM((rows, TILE), BF16),
                        pltpu.VMEM((2, TILE, D), F32), pltpu.VMEM((2, 4, 2, 192, TILE), F32),
                        pltpu.VMEM((4, TILE, D), F32), pltpu.VMEM((RING, 4, 192, TILE), F32),
                        pltpu.VMEM((2, 2, TILE, 768), F32), pltpu.VMEM((RING, 192, TILE), F32),
                        dma((2, 4)), dma((2,)), dma((2,)), dma((4,)), dma((RING,)), dma((4,)), dma((RING,)),
                        dma((2, 2)), dma((RING,)), dma((4,))] + ([] if mid else [pltpu.VMEM((rows, TILE), F32), pltpu.VMEM((rows, TILE), BF16), dma((2,))]),
        compiler_params=params(collective_id=int(mid), has_side_effects=True),
        cost_estimate=cost(4 if mid else 3, 300), name="middle" if mid else "last",
    )(a, b, *more)


def back_kernel(q_ref, w_ref, o_ref):
    o_ref[...] = dot_nt(q_ref[...], w_ref[...]).astype(BF16)


def back(q, w3):
    rows = q.shape[0]
    bm, bn = 512, 768
    return pl.pallas_call(
        back_kernel,
        grid=(D // bn, rows // bm),
        in_specs=[pl.BlockSpec((bm, FF), lambda j, i: (i, 0)), pl.BlockSpec((bn, FF), lambda j, i: (j, 0))],
        out_specs=pl.BlockSpec((bm, bn), lambda j, i: (i, j)),
        out_shape=jax.ShapeDtypeStruct((rows, D), BF16),
        compiler_params=params(), cost_estimate=cost(1, 130), name="back",
    )(q, w3)


def norm_kernel(*refs):
    *ins, o_ref, acc, one, all_v, send, recv = refs
    step = pl.program_id(0)
    me = lax.axis_index("data")

    @pl.when(step == 0)
    def _():
        bar = pltpu.get_barrier_semaphore()
        for k in range(1, 8):
            pl.semaphore_signal(bar, inc=1, device_id=((me + k) % 8,), device_id_type=MESH)
        pl.semaphore_wait(bar, 7)
        acc[...] = jnp.zeros_like(acc)

    for k in range(0, len(ins), 3):
        v = ins[k][...] + ins[k + 1][...] + ins[k + 2][...]
        v = v.reshape(v.shape[-2] // 8, 8, v.shape[-1])
        v = jnp.sum(v * v, axis=0)
        acc[...] += sum(v[:, i:i + 128] for i in range(0, v.shape[1], 128))

    @pl.when(step == TILES - 1)
    def _():
        one[...] = jnp.broadcast_to(jnp.sum(acc[...], keepdims=True), one.shape)
        copies = [pltpu.make_async_remote_copy(
            src_ref=one, dst_ref=all_v.at[me], send_sem=send.at[k], recv_sem=recv.at[me],
            device_id=((me + k) % 8,), device_id_type=MESH) for k in range(1, 8)]
        for c in copies:
            c.start()
        all_v[me] = one[...]
        for k in range(1, 8):
            src = (me + k) % 8
            pltpu.make_async_copy(all_v.at[src], all_v.at[src], recv.at[src]).wait()
        tot = all_v[0]
        for k in range(1, 8):
            tot = tot + all_v[k]
        o_ref[...] = tot
        for c in copies:
            c.wait_send()


def norm(parts4, parts3):
    four = pl.BlockSpec((1, 1, 64, 768), lambda s: (s // 12, s // 4 % 3, s % 4, 0))
    three = pl.BlockSpec((1, 192, TILE), lambda s: (s, 0, 0))
    one = pl.BlockSpec((8, 128), lambda s: (0, 0))
    dma = pltpu.SemaphoreType.DMA
    return pl.pallas_call(
        norm_kernel,
        grid=(TILES,),
        in_specs=[four] * len(parts4) + [three] * len(parts3),
        out_specs=one,
        out_shape=jax.ShapeDtypeStruct((8, 128), F32),
        scratch_shapes=[pltpu.VMEM((8, 128), F32), pltpu.VMEM((8, 128), F32), pltpu.VMEM((8, 8, 128), F32), dma((8,)), dma((8,))],
        compiler_params=params(collective_id=2, has_side_effects=True), name="norm",
    )(*parts4, *parts3)


def adam_kernel(tot_ref, lr_ref, clip_ref, a_ref, b_ref, c_ref, master_ref, mom_ref, vel_ref, dep, w_ref, master_out, mom_out, vel_out):
    n = jnp.sqrt(tot_ref[0:1, 0:1]) / 8
    scale = jnp.minimum(1.0, clip_ref[0, 0] / (n + NORM_EPS)) / 8
    g = a_ref[...] + b_ref[...] + c_ref[...]
    scaled = scale * g.reshape(g.shape[-2:])
    mom = BETA_ONE * mom_ref[...] + (1.0 - BETA_ONE) * scaled
    vel = BETA_TWO * vel_ref[...] + (1.0 - BETA_TWO) * scaled * scaled
    master = master_ref[...] - lr_ref[0, 0] * (mom / CORR_ONE) / (jnp.sqrt(vel / CORR_TWO) + EPSILON)
    w_ref[...] = master.astype(BF16)
    master_out[...] = master
    mom_out[...] = mom
    vel_out[...] = vel


def adam(tot, rate, clip, parts, master, mom, vel, dep):
    if parts[0].ndim == 4:
        src = pl.BlockSpec((1, 1, 256, 768), lambda s: (s % 2, s // 2, 0, 0))
        dst = pl.BlockSpec((256, 768), lambda s: (s // 2, s % 2))
        steps = 6
    else:
        src = pl.BlockSpec((1, 192, TILE), lambda s: (s, 0, 0))
        dst = pl.BlockSpec((192, TILE), lambda s: (0, tile(s)))
        steps = TILES
    one = pl.BlockSpec((8, 128), lambda s: (0, 0))
    flat = pl.BlockSpec(memory_space=pltpu.SMEM)
    return pl.pallas_call(
        adam_kernel,
        grid=(steps,),
        in_specs=[one, flat, flat] + [src] * 3 + [dst] * 3 + [ANY],
        out_specs=[dst] * 4,
        out_shape=[jax.ShapeDtypeStruct(master.shape, t) for t in (BF16, F32, F32, F32)],
        compiler_params=params(), name="adam",
    )(tot, rate, clip, *parts, master, mom, vel, dep)


def place_kernel(count, sub, at_ref, *refs):
    o_ref = refs[-1]
    step = pl.program_id(0)
    for k in range(count):
        @pl.when(step // sub == k)
        def _():
            o_ref[...] = refs[k][...]


def place_rows(at, ins, sub, shape, old=None):
    count = len(ins)
    rows, cols = ins[0].shape
    bm = rows // sub
    specs = [pl.BlockSpec((bm, cols), lambda s, at_ref, k=k: (jnp.clip(s - k * sub, 0, sub - 1), 0)) for k in range(count)]
    extra = [] if old is None else [old]
    return pl.pallas_call(
        functools.partial(place_kernel, count, sub),
        grid_spec=pltpu.PrefetchScalarGridSpec(
            num_scalar_prefetch=1, grid=(count * sub,), in_specs=specs + [ANY] * len(extra),
            out_specs=pl.BlockSpec((bm, cols), lambda s, at_ref: (at_ref[s // sub] * sub + s % sub, 0))),
        out_shape=jax.ShapeDtypeStruct(shape, BF16),
        input_output_aliases={} if old is None else {count + 1: 0},
        compiler_params=params(), name="rows",
    )(at, *ins, *extra)


def by_x(v):
    return lax.ppermute(v, "data", X_PAIRS)


def by_y(v):
    return lax.ppermute(v, "data", Y_PAIRS)


def by_core(v):
    return lax.ppermute(v, "data", C_PAIRS)


def gather(shards, order):
    me = lax.axis_index("data")
    near_at = me ^ jnp.arange(6)
    far_at = (me ^ jnp.array([6, 6, 7, 7])) * 2 + jnp.array([0, 1, 0, 1])
    full = [None] * 4
    diag = [None] * 4
    first = [(by_core(v), by_x(v), by_y(v)) for v in shards]
    for i in order:
        own = shards[i]
        own_c, at_x, at_y = first[i]
        half = own.shape[0] // 2
        diag[i] = by_y(at_x[:half]), by_x(at_y[half:])
        near = own, own_c, at_x, by_core(at_x), at_y, by_core(at_y)
        full[i] = place_rows(near_at, near, 1, (own.shape[0] * 8, own.shape[1]))
    diag, full = lax.optimization_barrier((diag, full))
    for i in order:
        far = *diag[i], by_core(diag[i][0]), by_core(diag[i][1])
        full[i] = place_rows(far_at, far, 1, full[i].shape, full[i])
    return full


def solution(mesh):
    groups = mesh.shape["data"]
    rows_spec = P("data", None)
    full_spec = P(None, None)
    scalar_spec = P()

    def shard_body(act_in, grad_out, w_up1, w_down1, w_up2, w_down2, master_up1, master_down1, master_up2, master_down2,
                   mom_up1, mom_down1, mom_up2, mom_down2, vel_up1, vel_down1, vel_up2, vel_down2, learn_rate, clip_norm):
        h1, z1, u = front(act_in, w_up1, w_down1)
        q2, *parts = fused(True, u, grad_out, w_up2, w_down2)
        eu = back(q2, w_up2)
        parts = list(parts) + list(fused(False, act_in, eu, w_down1, z1, h1))
        g_down2, g_up2, g_down1, g_up1 = [parts[k:k + 3] for k in range(0, 12, 3)]
        tot = norm(g_down2 + g_down1, g_up2 + g_up1)
        grad_norm = jnp.sqrt(tot[0, 0]) / groups
        grads = (g_up1, g_down1, g_up2, g_down2)
        masters = (master_up1, master_down1, master_up2, master_down2)
        moms = (mom_up1, mom_down1, mom_up2, mom_down2)
        vels = (vel_up1, vel_down1, vel_up2, vel_down2)
        rate, clip = learn_rate.reshape(1, 1), clip_norm.reshape(1, 1)
        states = [None] * 4
        dep = tot
        order = (1, 3, 0, 2)
        for i in order:
            states[i] = adam(tot, rate, clip, grads[i], masters[i], moms[i], vels[i], dep)
            dep = states[i][1]
        weights = gather([v[0] for v in states], order)
        results = weights
        for f in range(1, 4):
            results = results + [s[f] for s in states]
        return tuple(results + [grad_norm])

    in_specs = (rows_spec, rows_spec) + (full_spec,) * 4 + (rows_spec,) * 12 + (scalar_spec, scalar_spec)
    out_specs = (full_spec,) * 4 + (rows_spec,) * 12 + (scalar_spec,)
    return jax.shard_map(shard_body, mesh=mesh, in_specs=in_specs, out_specs=out_specs, check_vma=False)
```

```python
import functools
import math

import jax
import jax.numpy as jnp
from jax import lax
from jax.experimental import pallas as pl
from jax.experimental.pallas import tpu as pltpu
from jax.sharding import PartitionSpec as P

STEP = 20
BETA_ONE = 0.9
BETA_TWO = 0.95
EPSILON = 1e-8
NORM_EPS = 1e-6
CORR_ONE = 1.0 - BETA_ONE ** STEP
CORR_TWO = 1.0 - BETA_TWO ** STEP
ROOT_HALF = math.sqrt(0.5)
EXP_SCALE = -0.5 * math.log2(math.e)
EXP_SHIFT = -0.5 * math.log2(2.0 * math.pi)

F32 = jnp.float32
BF16 = jnp.bfloat16
MESH = pl.DeviceIdType.MESH
ANY = pl.BlockSpec(memory_space=pl.ANY)
VMEM_LIMIT = 67043328
D = 1536
FF = 6144
TILE = 256
X_PAIRS = [(i, i ^ 2) for i in range(8)]
Y_PAIRS = [(i, i ^ 4) for i in range(8)]
C_PAIRS = [(i, i ^ 1) for i in range(8)]


def dot_nn(a, b):
    return lax.dot_general(a, b, (((1,), (0,)), ((), ())), preferred_element_type=F32)


def dot_nt(a, b):
    return lax.dot_general(a, b, (((1,), (1,)), ((), ())), preferred_element_type=F32)


def dot_tn(a, b):
    return lax.dot_general(a, b, (((0,), (0,)), ((), ())), preferred_element_type=F32)


def normal_cdf(z):
    return 0.5 * lax.erf(z * ROOT_HALF) + 0.5


def gelu_slope(z, cdf):
    return cdf + z * jnp.exp2(z * z * EXP_SCALE + EXP_SHIFT)


def params(**kw):
    return pltpu.CompilerParams(vmem_limit_bytes=VMEM_LIMIT, **kw)


def cost(units, mib):
    return pl.CostEstimate(flops=int(units * 2 * 4096 * D * FF), bytes_accessed=mib * 2 ** 20, transcendentals=0)


def place():
    me = lax.axis_index("data")
    core = me % 2
    chip = me // 2
    return me, core, chip % 2, chip // 2


def front_kernel(x_ref, w1_hbm, w2_hbm, h_ref, z_ref, u_ref, w1_v, w2_v, sem):
    step = pl.program_id(0)
    n1, n2 = 1024, 512

    def loads():
        one = [pltpu.make_async_copy(w1_hbm.at[:, n:n + n1], w1_v.at[:, n:n + n1], sem.at[i])
               for i, n in enumerate(range(0, FF, n1))]
        two = [pltpu.make_async_copy(w2_hbm.at[:, n:n + n2], w2_v.at[:, n:n + n2], sem.at[FF // n1 + i])
               for i, n in enumerate(range(0, D, n2))]
        return one, two

    def work(first):
        one, two = loads()
        if first:
            for c in one + two:
                c.start()
        for n in range(0, FF, 512):
            if first and n % n1 == 0:
                one[n // n1].wait()
            z = dot_nn(x_ref[...], w1_v[:, n:n + 512])
            h_ref[:, n:n + 512] = (z * normal_cdf(z)).astype(BF16)
            z_ref[:, n:n + 512] = z
        for n in range(0, D, n2):
            if first:
                two[n // n2].wait()
            u_ref[:, n:n + n2] = dot_nn(h_ref[...], w2_v[:, n:n + n2]).astype(BF16)

    @pl.when(step == 0)
    def _():
        work(True)

    @pl.when(step > 0)
    def _():
        work(False)


def front(x, w1, w2):
    rows = x.shape[0]
    bm = 256
    return pl.pallas_call(
        front_kernel,
        grid=(rows // bm,),
        in_specs=[pl.BlockSpec((bm, D), lambda i: (i, 0)), ANY, ANY],
        out_specs=[pl.BlockSpec((bm, FF), lambda i: (i, 0)), pl.BlockSpec((bm, FF), lambda i: (i, 0)),
                   pl.BlockSpec((bm, D), lambda i: (i, 0))],
        out_shape=[jax.ShapeDtypeStruct((rows, FF), BF16), jax.ShapeDtypeStruct((rows, FF), F32),
                   jax.ShapeDtypeStruct((rows, D), BF16)],
        scratch_shapes=[pltpu.VMEM((D, FF), BF16), pltpu.VMEM((FF, D), BF16), pltpu.SemaphoreType.DMA((9,))],
        compiler_params=params(), cost_estimate=cost(2, 220), name="front",
    )(x, w1, w2)


TILES = 24
RING = 8


def fused_kernel(mid, a_hbm, b_hbm, w_ref, *rest):
    if mid:
        w4_ref, q_at, *rest = rest
    else:
        z_hbm, h_hbm, *rest = rest
        *rest, z_ref, h_at, tile_sem = rest
    (stay4, near4, fin4, stay3, near3, fin3, a_v, b_v, hidden_v, raw4, raw3, got4, got3, far4, far3,
     load_sem, send4, send3, recv4, recv3, done4, done3, recv_far4, recv_far3, recv_hbm) = rest
    if mid:
        h_at = hidden_v
    else:
        q_at = hidden_v
    step = pl.program_id(0)
    me, core, px, py = place()
    partner = me + 1 - 2 * core
    x_dev = me + 2 - 4 * px
    y_dev = me + 4 - 8 * py
    own_chip = py * 2 + px
    x_chip = py * 2 + 1 - px
    y_chip = (1 - py) * 2 + px
    part = 1024
    lag = 2 if mid else 4
    slack = RING - lag - 2

    def remote(src, dst, send, recv, dev):
        return pltpu.make_async_remote_copy(src_ref=src, dst_ref=dst, send_sem=send, recv_sem=recv,
                                            device_id=(dev,), device_id_type=MESH)

    def drain(ref, sem):
        pltpu.make_async_copy(ref, ref, sem).wait()

    def loads():
        return [[pltpu.make_async_copy(hbm.at[i:i + part], v.at[i:i + part], load_sem.at[k, i // part])
                 for i in range(0, 4096, part)] for k, (hbm, v) in enumerate(((a_hbm, a_v), (b_hbm, b_v)))]

    def columns(k, s):
        hbm, v = ((z_hbm, z_ref), (h_hbm, h_at))[k]
        return pltpu.make_async_copy(hbm.at[:, pl.ds(pl.multiple_of(tile_of(s) * TILE, TILE), TILE)], v, tile_sem.at[k])

    def following(k):
        if not mid:
            @pl.when(step + 1 < TILES)
            def _():
                columns(k, step + 1).start()

    def mine(s):
        return (s // 4) % 2 == core

    def role(s):
        return (s + px) % 2 + 2 * ((s // 2 + py) % 2)

    def share3(s):
        return remote(raw3.at[s % 2, :, 1 - core], got3.at[s % RING], send3.at[s % 2], recv3.at[s % RING], partner)

    def share4(s):
        return remote(raw4.at[s % 2], got4.at[s % 4], send4.at[s % 2], recv4.at[s % 4], partner)

    def legs3(s):
        odd = s % 2
        first = x_dev + odd * (y_dev - x_dev)
        second = y_dev + odd * (x_dev - y_dev)
        near = x_chip + odd * (y_chip - x_chip)
        far = y_chip + odd * (x_chip - y_chip)
        blk = got3.at[s % RING]
        sem = done3.at[s % RING]
        return (remote(blk.at[x_chip + y_chip - own_chip], far3.at[s % RING], sem, recv_far3.at[s % RING], first),
                remote(blk.at[near], near3.at[s], sem, recv_hbm.at[0], first),
                pltpu.make_async_copy(blk.at[own_chip], stay3.at[s], sem),
                remote(blk.at[far], fin3.at[s], sem, recv_hbm.at[1], second), far)

    def halves(s):
        return [(got4.at[s % 4, :, k * 768:k * 768 + 768], done4.at[s % 4]) for k in range(2)]

    def first4(s):
        t = s // 8
        r = role(s)
        for k, (blk, sem) in enumerate(halves(s)):
            dev = y_dev if k else x_dev

            @pl.when(r == 3)
            def _():
                remote(blk, far4.at[t % 2, k], sem, recv_far4.at[t % 2, k], dev).start()

            @pl.when(r == 1 + k)
            def _():
                remote(blk, near4.at[k, t], sem, recv_hbm.at[2], dev).start()

            @pl.when(r == 0)
            def _():
                pltpu.make_async_copy(blk, stay4.at[k, t], sem).start()

    def second4(s):
        t = s // 8
        r = role(s)
        for k, (blk, sem) in enumerate(halves(s)):
            @pl.when(r == 2 - k)
            def _():
                drain(far4.at[t % 2, k], recv_far4.at[t % 2, k])
                blk[...] = blk[...] + far4[t % 2, k]
                remote(blk, fin4.at[k, t], sem, recv_hbm.at[3], x_dev if k else y_dev).start()

    def add3(s):
        for q in range(4):
            got3[s % RING, q] = got3[s % RING, q] + raw3[s % 2, q, core]

    def fold3(s):
        far = legs3(s)[4]
        got3[s % RING, far] = got3[s % RING, far] + far3[s % RING]

    def hidden(first):
        cps = loads() if first else None
        if first and not mid:
            for k in range(2):
                columns(k, step).start()
        if first:
            for pair in zip(*cps):
                for c in pair:
                    c.start()
        if not mid:
            columns(0, step).wait()
        for i in range(0, 4096, 256):
            if first and i % part == 0:
                cps[1][i // part].wait()
                if mid:
                    cps[0][i // part].wait()
            rows = slice(i, i + 256)
            if mid:
                z = dot_nn(a_v[rows], w_ref[...])
                e = dot_nt(b_v[rows], w4_ref[...]).astype(BF16)
                cdf = normal_cdf(z)
                h_at[rows] = (z * cdf).astype(BF16)
            else:
                e = dot_nt(b_v[rows], w_ref[...]).astype(BF16)
                z = z_ref[rows]
                cdf = normal_cdf(z)
            q_at[rows] = (e.astype(F32) * gelu_slope(z, cdf)).astype(BF16)
        if first and not mid:
            for c in cps[0]:
                c.wait()
        following(0)

    def dot4():
        raw4[step % 2] = dot_tn(h_at[...], b_v[...])

    both = jnp.logical_and
    prev = step - 1
    old = prev - lag
    gone = old - slack
    live = step < TILES
    fresh = both(step >= 1, step <= TILES)

    @pl.when(step == 0)
    def _():
        bar = pltpu.get_barrier_semaphore()
        for dev in (partner, x_dev, y_dev):
            pl.semaphore_signal(bar, inc=1, device_id=(dev,), device_id_type=MESH)
        pl.semaphore_wait(bar, 3)
        hidden(True)

    @pl.when(both(step > 0, live))
    def _():
        hidden(False)

    @pl.when(both(step >= 2, step < TILES + 2))
    def _():
        share3(step - 2).wait_send()

        @pl.when(jnp.logical_not(mine(step - 2)))
        def _():
            share4(step - 2).wait_send()

    def settle(s):
        drain(got3.at[s % RING], done3.at[s % RING])

        @pl.when(mine(s))
        def _():
            drain(got4.at[s % 4], done4.at[s % 4])

    @pl.when(gone >= 0)
    def _():
        settle(gone)

    @pl.when(fresh)
    def _():
        share3(prev).wait_recv()

        @pl.when(mine(prev))
        def _():
            share4(prev).wait_recv()
            got4[prev % 4] = got4[prev % 4] + raw4[prev % 2]

    @pl.when(old >= 0)
    def _():
        drain(far3.at[old % RING], recv_far3.at[old % RING])

    if not mid:
        @pl.when(live)
        def _():
            columns(1, step).wait()

    @pl.when(both(old >= 0, live))
    def _():
        add3(prev)
        fold3(old)
        dot4()
        following(1)

    @pl.when(old < 0)
    def _():
        dot4()
        following(1)

    @pl.when(both(fresh, jnp.logical_or(old < 0, step == TILES)))
    def _():
        add3(prev)

    @pl.when(step >= TILES)
    def _():
        fold3(old)

    @pl.when(old >= 0)
    def _():
        legs3(old)[3].start()

        @pl.when(mine(old))
        def _():
            second4(old)

    @pl.when(fresh)
    def _():
        for c in legs3(prev)[:3]:
            c.start()

        @pl.when(mine(prev))
        def _():
            first4(prev)

    @pl.when(both(live, jnp.logical_not(mine(step))))
    def _():
        share4(step).start()

    @pl.when(live)
    def _():
        g3 = dot_tn(a_v[...], q_at[...])
        for q in range(4):
            for c in range(2):
                at = q * 384 + c * 192
                raw3[step % 2, q, c] = g3[at:at + 192]
        share3(step).start()

    @pl.when(step == TILES + lag)
    def _():
        for s in range(TILES - slack, TILES):
            settle(s)
        for k, ref in enumerate((near3, fin3, near4, fin4)):
            drain(ref, recv_hbm.at[k])


def tile_of(s):
    return (2 * (s % 4) + s // 4 % 2) * 3 + s // 8


def tile(s):
    return tile_of(jnp.minimum(s, TILES - 1))


def fused(mid, a, b, *more):
    rows = a.shape[0]

    down_w = pl.BlockSpec((TILE, D), lambda s: (tile(s), 0))
    up_w = pl.BlockSpec((D, TILE), lambda s: (0, tile(s)))
    wide = pl.BlockSpec((rows, TILE), lambda s: (0, tile(s)))
    g4 = jax.ShapeDtypeStruct((2, 3, 256, 768), F32)
    g3 = jax.ShapeDtypeStruct((TILES, 192, TILE), F32)
    dma = pltpu.SemaphoreType.DMA
    return pl.pallas_call(
        functools.partial(fused_kernel, mid),
        grid=(TILES + (3 if mid else 5),),
        in_specs=[ANY, ANY] + ([up_w, down_w] if mid else [down_w, ANY, ANY]),
        out_specs=([wide] if mid else []) + [ANY] * 6,
        out_shape=([jax.ShapeDtypeStruct((rows, FF), BF16)] if mid else []) + [g4] * 3 + [g3] * 3,
        scratch_shapes=[pltpu.VMEM((rows, D), BF16), pltpu.VMEM((rows, D), BF16), pltpu.VMEM((rows, TILE), BF16),
                        pltpu.VMEM((2, TILE, D), F32), pltpu.VMEM((2, 4, 2, 192, TILE), F32),
                        pltpu.VMEM((4, TILE, D), F32), pltpu.VMEM((RING, 4, 192, TILE), F32),
                        pltpu.VMEM((2, 2, TILE, 768), F32), pltpu.VMEM((RING, 192, TILE), F32),
                        dma((2, 4)), dma((2,)), dma((2,)), dma((4,)), dma((RING,)), dma((4,)), dma((RING,)),
                        dma((2, 2)), dma((RING,)), dma((4,))] + ([] if mid else [pltpu.VMEM((rows, TILE), F32), pltpu.VMEM((rows, TILE), BF16), dma((2,))]),
        compiler_params=params(collective_id=int(mid), has_side_effects=True),
        cost_estimate=cost(4 if mid else 3, 300), name="middle" if mid else "last",
    )(a, b, *more)


def back_kernel(q_ref, w_ref, o_ref):
    o_ref[...] = dot_nt(q_ref[...], w_ref[...]).astype(BF16)


def back(q, w3):
    rows = q.shape[0]
    bm, bn = 512, 768
    return pl.pallas_call(
        back_kernel,
        grid=(D // bn, rows // bm),
        in_specs=[pl.BlockSpec((bm, FF), lambda j, i: (i, 0)), pl.BlockSpec((bn, FF), lambda j, i: (j, 0))],
        out_specs=pl.BlockSpec((bm, bn), lambda j, i: (i, j)),
        out_shape=jax.ShapeDtypeStruct((rows, D), BF16),
        compiler_params=params(), cost_estimate=cost(1, 130), name="back",
    )(q, w3)


def norm_kernel(*refs):
    *ins, o_ref, acc, one, all_v, send, recv = refs
    step = pl.program_id(0)
    me = lax.axis_index("data")

    @pl.when(step == 0)
    def _():
        bar = pltpu.get_barrier_semaphore()
        for k in range(1, 8):
            pl.semaphore_signal(bar, inc=1, device_id=((me + k) % 8,), device_id_type=MESH)
        pl.semaphore_wait(bar, 7)
        acc[...] = jnp.zeros_like(acc)

    for k in range(0, len(ins), 3):
        v = ins[k][...] + ins[k + 1][...] + ins[k + 2][...]
        v = v.reshape(-1, 8, v.shape[-1])
        v = jnp.sum(v * v, axis=0)
        acc[...] += sum(v[:, i:i + 128] for i in range(0, v.shape[1], 128))

    @pl.when(step == TILES // 2 - 1)
    def _():
        one[...] = jnp.broadcast_to(jnp.sum(acc[...], keepdims=True), one.shape)
        copies = [pltpu.make_async_remote_copy(
            src_ref=one, dst_ref=all_v.at[me], send_sem=send.at[k], recv_sem=recv.at[me],
            device_id=((me + k) % 8,), device_id_type=MESH) for k in range(1, 8)]
        for c in copies:
            c.start()
        all_v[me] = one[...]
        for k in range(1, 8):
            src = (me + k) % 8
            pltpu.make_async_copy(all_v.at[src], all_v.at[src], recv.at[src]).wait()
        tot = all_v[0]
        for k in range(1, 8):
            tot = tot + all_v[k]
        o_ref[...] = tot
        for c in copies:
            c.wait_send()


def norm(parts4, parts3):
    four = pl.BlockSpec((1, 1, 128, 768), lambda s: (s // 6, s // 2 % 3, s % 2, 0))
    three = pl.BlockSpec((2, 192, TILE), lambda s: (s, 0, 0))
    one = pl.BlockSpec((8, 128), lambda s: (0, 0))
    dma = pltpu.SemaphoreType.DMA
    return pl.pallas_call(
        norm_kernel,
        grid=(TILES // 2,),
        in_specs=[four] * len(parts4) + [three] * len(parts3),
        out_specs=one,
        out_shape=jax.ShapeDtypeStruct((8, 128), F32),
        scratch_shapes=[pltpu.VMEM((8, 128), F32), pltpu.VMEM((8, 128), F32), pltpu.VMEM((8, 8, 128), F32), dma((8,)), dma((8,))],
        compiler_params=params(collective_id=2, has_side_effects=True), name="norm",
    )(*parts4, *parts3)


def adam_kernel(tot_ref, lr_ref, clip_ref, a_ref, b_ref, c_ref, master_ref, mom_ref, vel_ref, dep, w_ref, master_out, mom_out, vel_out):
    n = jnp.sqrt(tot_ref[0:1, 0:1]) / 8
    scale = jnp.minimum(1.0, clip_ref[0, 0] / (n + NORM_EPS)) / 8
    g = a_ref[...] + b_ref[...] + c_ref[...]
    scaled = scale * g.reshape(g.shape[-2:])
    mom = BETA_ONE * mom_ref[...] + (1.0 - BETA_ONE) * scaled
    vel = BETA_TWO * vel_ref[...] + (1.0 - BETA_TWO) * scaled * scaled
    master = master_ref[...] - lr_ref[0, 0] * (mom / CORR_ONE) / (jnp.sqrt(vel / CORR_TWO) + EPSILON)
    w_ref[...] = master.astype(BF16)
    master_out[...] = master
    mom_out[...] = mom
    vel_out[...] = vel


def adam(tot, rate, clip, parts, master, mom, vel, dep):
    if parts[0].ndim == 4:
        src = pl.BlockSpec((1, 1, 256, 768), lambda s: (s % 2, s // 2, 0, 0))
        dst = pl.BlockSpec((256, 768), lambda s: (s // 2, s % 2))
        steps = 6
    else:
        src = pl.BlockSpec((1, 192, TILE), lambda s: (s, 0, 0))
        dst = pl.BlockSpec((192, TILE), lambda s: (0, tile(s)))
        steps = TILES
    one = pl.BlockSpec((8, 128), lambda s: (0, 0))
    flat = pl.BlockSpec(memory_space=pltpu.SMEM)
    return pl.pallas_call(
        adam_kernel,
        grid=(steps,),
        in_specs=[one, flat, flat] + [src] * 3 + [dst] * 3 + [ANY],
        out_specs=[dst] * 4,
        out_shape=[jax.ShapeDtypeStruct(master.shape, t) for t in (BF16, F32, F32, F32)],
        compiler_params=params(), cost_estimate=cost(0.15, 47), name="adam",
    )(tot, rate, clip, *parts, master, mom, vel, dep)


def place_kernel(count, sub, at_ref, *refs):
    o_ref = refs[-1]
    step = pl.program_id(0)
    for k in range(count):
        @pl.when(step // sub == k)
        def _():
            o_ref[...] = refs[k][...]


def place_rows(at, ins, sub, shape, old=None):
    count = len(ins)
    rows, cols = ins[0].shape
    bm = rows // sub
    specs = [pl.BlockSpec((bm, cols), lambda s, at_ref, k=k: (jnp.clip(s - k * sub, 0, sub - 1), 0)) for k in range(count)]
    extra = [] if old is None else [old]
    return pl.pallas_call(
        functools.partial(place_kernel, count, sub),
        grid_spec=pltpu.PrefetchScalarGridSpec(
            num_scalar_prefetch=1, grid=(count * sub,), in_specs=specs + [ANY] * len(extra),
            out_specs=pl.BlockSpec((bm, cols), lambda s, at_ref: (at_ref[s // sub] * sub + s % sub, 0))),
        out_shape=jax.ShapeDtypeStruct(shape, BF16),
        input_output_aliases={} if old is None else {count + 1: 0},
        compiler_params=params(), name="rows",
    )(at, *ins, *extra)


def by_x(v):
    return lax.ppermute(v, "data", X_PAIRS)


def by_y(v):
    return lax.ppermute(v, "data", Y_PAIRS)


def by_core(v):
    return lax.ppermute(v, "data", C_PAIRS)


def gather(shards, order):
    me = lax.axis_index("data")
    near_at = me ^ jnp.arange(6)
    far_at = (me ^ jnp.array([6, 6, 7, 7])) * 2 + jnp.array([0, 1, 0, 1])
    full = [None] * 4
    diag = [None] * 4
    first = [(by_core(v), by_x(v), by_y(v)) for v in shards]
    for i in order:
        own = shards[i]
        own_c, at_x, at_y = first[i]
        half = own.shape[0] // 2
        diag[i] = by_y(at_x[:half]), by_x(at_y[half:])
        near = own, own_c, at_x, by_core(at_x), at_y, by_core(at_y)
        full[i] = place_rows(near_at, near, 1, (own.shape[0] * 8, own.shape[1]))
    diag, full = lax.optimization_barrier((diag, full))
    for i in order:
        far = *diag[i], by_core(diag[i][0]), by_core(diag[i][1])
        full[i] = place_rows(far_at, far, 1, full[i].shape, full[i])
    return full


def solution(mesh):
    groups = mesh.shape["data"]
    rows_spec = P("data", None)
    full_spec = P(None, None)
    scalar_spec = P()

    def shard_body(act_in, grad_out, w_up1, w_down1, w_up2, w_down2, master_up1, master_down1, master_up2, master_down2,
                   mom_up1, mom_down1, mom_up2, mom_down2, vel_up1, vel_down1, vel_up2, vel_down2, learn_rate, clip_norm):
        h1, z1, u = front(act_in, w_up1, w_down1)
        q2, *parts = fused(True, u, grad_out, w_up2, w_down2)
        eu = back(q2, w_up2)
        parts = list(parts) + list(fused(False, act_in, eu, w_down1, z1, h1))
        g_down2, g_up2, g_down1, g_up1 = [parts[k:k + 3] for k in range(0, 12, 3)]
        tot = norm(g_down2 + g_down1, g_up2 + g_up1)
        grad_norm = jnp.sqrt(tot[0, 0]) / groups
        grads = (g_up1, g_down1, g_up2, g_down2)
        masters = (master_up1, master_down1, master_up2, master_down2)
        moms = (mom_up1, mom_down1, mom_up2, mom_down2)
        vels = (vel_up1, vel_down1, vel_up2, vel_down2)
        rate, clip = learn_rate.reshape(1, 1), clip_norm.reshape(1, 1)
        states = [None] * 4
        dep = tot
        order = (1, 3, 0, 2)
        for i in order:
            states[i] = adam(tot, rate, clip, grads[i], masters[i], moms[i], vels[i], dep)
            dep = states[i][1]
        weights = gather([v[0] for v in states], order)
        results = weights
        for f in range(1, 4):
            results = results + [s[f] for s in states]
        return tuple(results + [grad_norm])

    in_specs = (rows_spec, rows_spec) + (full_spec,) * 4 + (rows_spec,) * 12 + (scalar_spec, scalar_spec)
    out_specs = (full_spec,) * 4 + (rows_spec,) * 12 + (scalar_spec,)
    return jax.shard_map(shard_body, mesh=mesh, in_specs=in_specs, out_specs=out_specs, check_vma=False)
```
